32 devices in a mesh: tok: 8 (over z, y), voc: 4 (over x, core).
Axes of the slice: x: 2, y: 2, z: 4, core: 2. Of those that a mesh axis runs over, the one named last changes fastest.
Arguments:
- hidden: bfloat16 [1024, 2048], P('tok'), may hold values from -6 to 6
- mix_weight: bfloat16 [4, 2048], P(None, 'voc'), may hold values from -0.0546875 to 0.0546875
- comp_proj: bfloat16 [2048, 4, 2048], P(None, None, 'voc'), may hold values from -0.110485435 to 0.110485435
- vocab_weight: bfloat16 [2048, 1024], P(None, 'voc'), may hold values from -0.625 to 0.625
- log_normalizer: float32 [4, 1024], P(None, 'tok'), may hold values from 11 to 11.6
- targets: int32 [1024], P('tok'), may hold values from 0 to 1023
- loss_grad: float32 [1024], P('tok'), may hold values from 0.5 to 1.5
Outputs:
- hidden_grad: bfloat16 [1024, 2048], P('tok', 'voc')
- proj_grad: bfloat16 [2048, 4, 2048], P('tok', None, 'voc')
- vocab_grad: bfloat16 [2048, 1024], P('tok', 'voc')
The draws below stay inside these ranges and needn't reach their ends.
All inputs are finite; a program needn't handle non-finite values.
Results may differ from the reference program's by a relative error of at most 0.02.
Values may be sent and summed in bfloat16 or wider, within the bound.
No kernel may reach another device: no remote copies, remote signals or barrier semaphores. Data moves between devices by JAX's collectives and lax.ppermute only.
A program may use at most 64 MiB of HBM per device.

```python
import jax
import jax.numpy as jnp
from jax import lax

D = 2048
K = 4
TOK_DEV = 128
V_DEV = 256
TOKENS = 1024
VOCAB = 1024
N_TOK = 8
N_VOC = 4


def draw_comp_proj(key, part):
    base_key = jax.random.fold_in(key, 11)
    noise_key = jax.random.fold_in(key, 12)
    shared = jax.random.truncated_normal(base_key, -4.0, 4.0, (D, 1, D), jnp.float32)
    private = jax.random.truncated_normal(noise_key, -4.0, 4.0, (D, K, D), jnp.float32)
    values = (0.98869 * shared + 0.15 * private) * D ** (-0.5)
    return values.astype(jnp.bfloat16)


def set_ends(array, stream_key, low, top_value):
    longest = array.shape.index(max(array.shape))
    spots = []
    for shift in (0, 1):
        where = [jax.random.randint(jax.random.fold_in(stream_key, axis), (), 0, length) for axis, length in enumerate(array.shape)]
        where[longest] = (where[longest] + shift) % array.shape[longest]
        spots.append(tuple(where))
    return array.at[spots[0]].set(low).at[spots[1]].set(top_value)


def level_of(key, shape, cuts, smallest, high):
    def one(position, parts):
        heights = jax.random.uniform(jax.random.fold_in(jax.random.fold_in(key, 6), position), (parts,), jnp.float32, smallest / len(cuts), high / len(cuts))
        return jnp.repeat(jnp.exp(heights), shape[position] // parts).reshape((-1,) + (1,) * (len(shape) - position - 1))

    level = one(*cuts[0])
    for cut in cuts[1:]:
        level = level * one(*cut)
    return level


def noise(key, extent, width, reach, split=(), kind=jnp.bfloat16):
    entries = jax.random.normal(key, extent, jnp.float32) * width
    if len(split) > 0:
        entries = level_of(key, extent, split, -0.22, 0.18) * entries
    return jnp.clip(entries, min=-reach, max=reach).astype(kind)


def setup_inputs(seed: int = 0) -> dict:
    key_of = jax.random.split(jax.random.key(seed), 8)
    hidden = noise(key_of[0], (TOKENS, D), 1.0, 6.0, ((0, 8),))
    mix_weight = noise(key_of[1], (K, D), (6 * D) ** -0.5, 0.0546875, ((1, 4),))
    comp_proj = draw_comp_proj(jax.random.fold_in(key_of[7], 71), 0)
    vocab_weight = noise(key_of[3], (D, VOCAB), 0.1, 0.625, ((1, 4),))
    log_normalizer = jnp.clip(11.0 + 0.6000004 * jax.random.uniform(key_of[4], (K, TOKENS), jnp.float32) ** level_of(key_of[4], (K, TOKENS), ((1, 8),), -0.2, 0.2), 11.0, 11.6)
    targets = set_ends(jax.random.randint(key_of[5], (TOKENS,), 0, VOCAB), jax.random.fold_in(key_of[5], 1), 0, VOCAB - 1).astype(jnp.int32)
    loss_grad = jnp.clip(0.5 + 1.0 * jax.random.uniform(key_of[6], (TOKENS,), jnp.float32) ** level_of(key_of[6], (TOKENS,), ((0, 8),), -0.2, 0.2), 0.5, 1.5)
    return {"hidden": hidden, "mix_weight": mix_weight, "comp_proj": comp_proj, "vocab_weight": vocab_weight, "log_normalizer": log_normalizer, "targets": targets, "loss_grad": loss_grad}


def rounded(values):
    return lax.optimization_barrier(values.astype(jnp.bfloat16)).astype(jnp.float32)


def reference(hidden, mix_weight, comp_proj, vocab_weight, log_normalizer, targets, loss_grad):
    highest = lax.Precision.HIGHEST
    weight_full = vocab_weight.astype(jnp.float32)
    proj_full = comp_proj.astype(jnp.float32)
    mix_full = mix_weight.astype(jnp.float32)
    vocab_ids = jnp.arange(VOCAB, dtype=jnp.int32)
    hidden_groups = hidden.reshape(N_TOK, TOK_DEV, D)
    norm_groups = jnp.transpose(log_normalizer.reshape(K, N_TOK, TOK_DEV), (1, 0, 2))
    target_groups = targets.reshape(N_TOK, TOK_DEV)
    cotangent_groups = loss_grad.reshape(N_TOK, TOK_DEV)

    def one_group(running, inputs):
        vocab_sum, proj_sum = running
        states, normalizer, wanted, cotangent = inputs
        states_f = states.astype(jnp.float32)
        contexts = jnp.tanh(jnp.einsum("td,dke->tke", states_f, proj_full, precision=highest)).astype(jnp.bfloat16)
        context_f = contexts.astype(jnp.float32)
        logits = jnp.einsum("tkd,dv->ktv", context_f, weight_full, precision=highest)
        mixing = jnp.einsum("td,kd->kt", states_f, mix_full, precision=highest)
        onehot = (wanted[:, None] == vocab_ids[None, :]).astype(jnp.float32)
        target = jnp.sum(logits * onehot[None], axis=2)
        exp_mix = jnp.exp(mixing)
        weights = exp_mix / jnp.sum(exp_mix, axis=0, keepdims=True)
        likely = jnp.exp(target - normalizer)
        joint_mass = weights * likely
        posterior = joint_mass / jnp.sum(joint_mass, axis=0, keepdims=True)
        factor = cotangent[None, :] * posterior
        logit_grad = (factor[:, :, None] * (jnp.exp(logits - normalizer[:, :, None]) - onehot[None])).astype(jnp.bfloat16)
        mixing_grad = cotangent[None, :] * (weights - posterior)
        grad_f = logit_grad.astype(jnp.float32)
        vocab_part = jnp.einsum("tkd,ktv->dv", context_f, grad_f, precision=highest)
        vocab_sum = vocab_sum + rounded(vocab_part)
        blocks = jnp.einsum("ktbv,dbv->btkd", grad_f.reshape(K, TOK_DEV, N_VOC, V_DEV), weight_full.reshape(D, N_VOC, V_DEV), precision=highest)
        context_grad = jnp.sum(rounded(blocks), axis=0)
        pre_grad = rounded(context_grad * (1.0 - context_f * context_f))
        hidden_grad = (jnp.einsum("tke,jke->tj", pre_grad, proj_full, precision=highest) + jnp.einsum("kt,kd->td", mixing_grad, mix_full, precision=highest)).astype(jnp.bfloat16)
        proj_sum = proj_sum + jnp.einsum("tj,tke->jke", states_f, pre_grad, precision=highest)
        return (vocab_sum, proj_sum), hidden_grad

    start_state = (jnp.zeros((D, VOCAB), jnp.float32), jnp.zeros((D, K, D), jnp.float32))
    final_state, hidden_grads = lax.scan(one_group, start_state, (hidden_groups, norm_groups, target_groups, cotangent_groups))
    vocab_sum, proj_sum = final_state
    return hidden_grads.reshape(TOKENS, D), proj_sum.astype(jnp.bfloat16), vocab_sum.astype(jnp.bfloat16)
```

```python
import jax
import jax.numpy as jnp
from jax import lax
from jax.sharding import PartitionSpec as P

F32 = jnp.float32
BF16 = jnp.bfloat16
DOWN = 2.0**-32
UP = 2.0**32


def folded_ring(length):
    return [0] + list(range(1, length, 2)) + list(range(length - 2 + length % 2, 0, -2))


def dot(a, b, dims):
    return lax.dot_general(a, b, (dims, ((), ())), preferred_element_type=F32)


def body_pairs(n_tok, n_voc, hidden, mix_weight, comp_proj, vocab_weight, log_normalizer, targets, loss_grad):
    comps = comp_proj.shape[1]
    cols = comp_proj.shape[2]
    own_vocab = vocab_weight.shape[1]
    n_z = n_tok // 2
    voc = lax.axis_index("voc")
    tok = lax.axis_index("tok")
    z, y = tok // 2, tok % 2
    rows = hidden.shape[1] // n_tok
    ring = folded_ring(n_z)
    place_of = [ring.index(i) for i in range(n_z)]

    def swap_voc(x, bit):
        return lax.ppermute(x, "voc", [(i, i ^ bit) for i in range(n_voc)])

    def swap_tok(x, bit):
        return lax.ppermute(x, "tok", [(i, i ^ bit) for i in range(n_tok)])

    def along_ring(x, step):
        pairs = []
        for i in range(n_tok):
            to = ring[(place_of[i // 2] + step) % n_z]
            pairs.append((i, to * 2 + i % 2))
        return lax.ppermute(x, "tok", pairs)

    def ring_row(step):
        table = jnp.array([ring[(place_of[i] + step) % n_z] for i in range(n_z)], jnp.int32)
        return lax.dynamic_index_in_dim(table, z, keepdims=False)

    weight = jnp.concatenate([vocab_weight, swap_voc(vocab_weight, 1)], axis=1)
    weight_of = [lax.dynamic_slice_in_dim(weight, (voc ^ j) * cols, cols, 0) for j in range(n_voc)]

    hidden_of = []
    for step in range(n_z):
        block = ring_row(step) * 2
        mine = lax.dynamic_slice_in_dim(hidden, (block + y) * rows, rows, 1)
        other = lax.dynamic_slice_in_dim(hidden, (block + 1 - y) * rows, rows, 1)
        piece = jnp.concatenate([mine, other], axis=1)
        hidden_of.append(along_ring(piece, step) if step else piece)

    own_hidden = lax.dynamic_slice_in_dim(hidden, voc * cols, cols, 1)
    mixing = dot(mix_weight, own_hidden, ((1,), (1,)))
    mixing = mixing + swap_voc(mixing, 1)
    mixing = mixing + swap_voc(mixing, 2)
    exp_mix = jnp.exp(mixing)
    weights = exp_mix / jnp.sum(exp_mix, axis=0, keepdims=True)

    half = cols // 2
    context = [[None, None] for _ in range(n_voc)]
    for h in range(2):
        pre_act = jnp.einsum(
            "td,dke->kte", hidden, comp_proj[:, :, h * half : (h + 1) * half], preferred_element_type=F32
        )
        own = jnp.tanh(pre_act).astype(BF16)
        context[0][h] = own
        context[2][h] = swap_voc(own, 2)
        context[1][h] = swap_voc(own, 1)
        context[3][h] = swap_voc(context[2][h], 1)
    logits = 0.0
    for j in range(n_voc):
        for h in range(2):
            logits = logits + jnp.einsum(
                "kte,ev->ktv", context[j][h], weight_of[j][h * half : (h + 1) * half], preferred_element_type=F32
            )
    near = jnp.concatenate(
        [voc * own_vocab + lax.iota(jnp.int32, own_vocab), (voc ^ 1) * own_vocab + lax.iota(jnp.int32, own_vocab)]
    )
    onehot = (targets[:, None] == near[None, :]).astype(F32)
    target = jnp.sum(logits * onehot[None], axis=2)
    target = target + swap_voc(target, 2)
    excess = jnp.exp(logits - log_normalizer[:, :, None]) - onehot[None]
    scaled = (excess * DOWN).astype(BF16)
    likely = jnp.exp(target - log_normalizer)
    joint_mass = weights * likely
    posterior = joint_mass / jnp.sum(joint_mass, axis=0, keepdims=True)
    factor = loss_grad[None, :] * posterior
    mixing_grad = loss_grad[None, :] * (weights - posterior)

    pre_grads = []
    pieces = []
    for k in range(comps):
        away = dot(scaled[k], weight_of[2], ((1,), (1,))).astype(BF16)
        home = dot(scaled[k], weight_of[0], ((1,), (1,)))
        total = home + swap_voc(away, 2).astype(F32)
        own_f = jnp.concatenate([context[0][0][k], context[0][1][k]], axis=1).astype(F32)
        pre = ((total * factor[k][:, None]) * UP * (1.0 - own_f * own_f)).astype(BF16)
        pre_grads.append(pre)
        got = [pre]
        for _ in range(n_z - 1):
            got.append(along_ring(got[-1], 1))
        part = 0.0
        for step in range(n_z):
            part = part + dot(hidden_of[step], got[step], ((0,), (0,)))
        pieces.append(part[:rows] + swap_tok(part[rows:].astype(BF16), 1).astype(F32))
    proj_grad = jnp.stack([p.astype(BF16) for p in pieces], axis=1)

    pre_all = jnp.stack(pre_grads, axis=0)
    partial = jnp.einsum("kte,jke->tj", pre_all, comp_proj, preferred_element_type=F32).astype(BF16)
    block_of = [lax.dynamic_slice_in_dim(partial, (voc ^ j) * cols, cols, 1) for j in range(n_voc)]
    over = swap_voc(jnp.stack([block_of[1], block_of[3]]), 1).astype(F32)
    home = block_of[0].astype(F32) + over[0]
    away = (block_of[2].astype(F32) + over[1]).astype(BF16)
    hidden_sum = home + swap_voc(away, 2).astype(F32)
    mix_term = jnp.einsum(
        "kt,kd->td", mixing_grad, mix_weight.astype(F32), precision=lax.Precision.HIGHEST
    )
    hidden_grad = (hidden_sum + mix_term).astype(BF16)

    logit_grad = (factor[:, :, None] * excess[:, :, :own_vocab]).astype(BF16)
    parts = []
    for j in range(n_voc):
        for h in range(2):
            parts.append(
                jnp.einsum("kte,ktv->ev", context[j][h], logit_grad, preferred_element_type=F32).astype(BF16)
            )
    left = jnp.concatenate(parts, axis=0).reshape(n_voc, 2, rows, own_vocab)

    def halve(x, axis, bit, distance):
        keep = lax.dynamic_index_in_dim(x, bit, axis, keepdims=False).astype(F32)
        give = lax.dynamic_index_in_dim(x, 1 - bit, axis, keepdims=False)
        return (keep + swap_tok(give, distance).astype(F32)).astype(BF16)

    left = halve(left, 1, y, 1).reshape(2, 2, rows, own_vocab)
    left = halve(left, 1, (voc ^ z) & 1, 2)
    vocab_grad = halve(left, 0, ((voc ^ z) >> 1) & 1, 4)
    return (hidden_grad, proj_grad, vocab_grad)


def body_any(hidden, mix_weight, comp_proj, vocab_weight, log_normalizer, targets, loss_grad):
    voc_place = lax.axis_index("voc")
    own_cols = comp_proj.shape[2]
    own_vocab = vocab_weight.shape[1]
    pre_act = jnp.einsum("td,dke->ekt", hidden, comp_proj, preferred_element_type=F32)
    context_own = jnp.tanh(pre_act).astype(BF16)
    own_hidden = lax.dynamic_slice_in_dim(hidden, voc_place * own_cols, own_cols, 1)
    mixing_part = jnp.einsum("kd,td->kt", mix_weight, own_hidden, preferred_element_type=F32)
    mixing = lax.psum(mixing_part, "voc")
    context_full = lax.all_gather(context_own, "voc", axis=0, tiled=True)
    logits = jnp.einsum("dkt,dv->ktv", context_full, vocab_weight, preferred_element_type=F32)
    vocab_ids = voc_place * own_vocab + lax.iota(jnp.int32, own_vocab)
    onehot = (targets[:, None] == vocab_ids[None, :]).astype(F32)
    target = lax.psum(jnp.sum(logits * onehot[None], axis=2), "voc")
    exp_mix = jnp.exp(mixing)
    weights = exp_mix / jnp.sum(exp_mix, axis=0, keepdims=True)
    likely = jnp.exp(target - log_normalizer)
    joint_mass = weights * likely
    posterior = joint_mass / jnp.sum(joint_mass, axis=0, keepdims=True)
    factor = loss_grad[None, :] * posterior
    logit_grad = (
        factor[:, :, None] * (jnp.exp(logits - log_normalizer[:, :, None]) - onehot[None])
    ).astype(BF16)
    mixing_grad = loss_grad[None, :] * (weights - posterior)

    def scattered(x, axis):
        return lax.psum_scatter(x.astype(BF16), axis, scatter_dimension=0, tiled=True)

    vocab_grad = scattered(
        jnp.einsum("dkt,ktv->dv", context_full, logit_grad, preferred_element_type=F32), "tok"
    )
    context_grad = scattered(
        jnp.einsum("dv,ktv->dkt", vocab_weight, logit_grad, preferred_element_type=F32), "voc"
    ).astype(F32)
    own_f = context_own.astype(F32)
    pre_grad = (context_grad * (1.0 - own_f * own_f)).astype(BF16)
    hidden_sum = scattered(
        jnp.einsum("jke,ekt->jt", comp_proj, pre_grad, preferred_element_type=F32), "voc"
    ).astype(F32)
    mix_term = jnp.einsum(
        "kt,kd->td", mixing_grad, mix_weight.astype(F32), precision=lax.Precision.HIGHEST
    )
    hidden_grad = (hidden_sum.T + mix_term).astype(BF16)
    hidden_rows = lax.all_to_all(hidden, "tok", split_axis=1, concat_axis=0, tiled=True)
    proj_sum = jnp.einsum(
        "tr,ekt->rke",
        hidden_rows,
        lax.all_gather(pre_grad, "tok", axis=2, tiled=True),
        preferred_element_type=F32,
    )
    return (hidden_grad, proj_sum.astype(BF16), vocab_grad)


def solution(mesh):
    in_specs = (
        P("tok", None),
        P(None, "voc"),
        P(None, None, "voc"),
        P(None, "voc"),
        P(None, "tok"),
        P("tok"),
        P("tok"),
    )
    out_specs = (P("tok", "voc"), P("tok", None, "voc"), P("tok", "voc"))
    n_tok, n_voc = mesh.shape["tok"], mesh.shape["voc"]
    if n_voc == 4 and n_tok == 2 * n_voc:

        def body(*args):
            return body_pairs(n_tok, n_voc, *args)
    else:
        body = body_any
    return jax.shard_map(body, mesh=mesh, in_specs=in_specs, out_specs=out_specs, check_vma=False)
```
